32 devices in a mesh: grp: 4 (over y, x), dev: 8 (over z, core).
Axes of the slice: x: 2, y: 2, z: 4, core: 2. Of those that a mesh axis runs over, the one named last changes fastest.
Arguments:
- feeder_state: float32 [3072, 24, 256], P(('grp', 'dev')), may hold values from -6 to 6
- feeder_load: bfloat16 [3072, 24, 256], P(('grp', 'dev')), may hold values from -6 to 6
- feeder_inverse: bfloat16 [3072, 256, 256], P(('grp', 'dev')), as said below
- coupling: bfloat16 [3072, 256], P(('grp', 'dev')), may hold values from -0.375 to 0.375
- feeder_bus: int32 [3072], P(('grp', 'dev')), may hold values from 0 to 4095
- bus_coupling: bfloat16 [4096, 4096], P(('grp', 'dev')), may hold values from -0.1875 to 0.1875
- bus_diagonal: float32 [4096], P(('grp', 'dev')), may hold values from 1 to 3
- bus_load: float32 [24, 4096], P(None, ('grp', 'dev')), may hold values from -6 to 6
- bus_state: float32 [24, 4096], P(None, ('grp', 'dev')), may hold values from -6 to 6
- barrier: float32 [2], replicated, may hold values from 0.5 to 4
- step_length: float32 [2], replicated, may hold values from 0.4 to 1
Outputs:
- feeder_final: float32 [3072, 24, 256], P(('grp', 'dev'))
- bus_final: float32 [24, 4096], P(None, ('grp', 'dev'))
The draws below stay inside these ranges and needn't reach their ends.
Inputs may be any that keep to these rules, and one draw needn't show every extreme that they name: `feeder_inverse`: each block is symmetric with a positive diagonal and is positive definite.
All inputs are finite; a program needn't handle non-finite values.
Results may differ from the reference program's by a relative error of at most 0.0022.
Values may be sent and summed in bfloat16 or wider, within the bound.
No kernel may reach another device: no remote copies, remote signals or barrier semaphores. Data moves between devices by JAX's collectives and lax.ppermute only.
A program may use at most 128 MiB of HBM per device.

```python
import math
import jax
import jax.numpy as jnp
from jax import lax

NODES = 256
HOURS = 24
ITERS = 2
FEED_DEV = 96
FEEDERS = 3072
BUSES = 4096


def draw_feeder_inverse(key, part):
    first_key, second_key = jax.random.split(key)
    noise = jax.random.normal(first_key, (FEEDERS, NODES, NODES), jnp.float32)
    noise = noise / jnp.sqrt(jnp.float32(NODES))
    symmetric = 0.5 * (noise + jnp.swapaxes(noise, 1, 2))
    pivots = jax.random.uniform(second_key, (FEEDERS, NODES), jnp.float32, 2.0, 4.0)
    return (symmetric + pivots[:, :, None] * jnp.eye(NODES, dtype=jnp.float32)).astype(jnp.bfloat16)


def place_ends(entries, key, least, top_value):
    index_at = [jax.random.randint(jax.random.fold_in(key, axis), (), 0, length) for axis, length in enumerate(entries.shape)]
    longest = entries.shape.index(max(entries.shape))
    beside = index_at[:longest] + [(index_at[longest] + 1) % entries.shape[longest]] + index_at[longest + 1:]
    return entries.at[tuple(index_at)].set(least).at[tuple(beside)].set(top_value)


def block_levels(key, extent, shards, least, top_value):
    level, own = 1.0, jax.random.fold_in(key, 6)
    for position, parts in shards:
        heights = jnp.exp(jax.random.uniform(jax.random.fold_in(own, position), (parts,), jnp.float32, least / len(shards), top_value / len(shards)))
        level = level * jnp.repeat(heights, extent[position] // parts).reshape([-1 if axis == position else 1 for axis in range(len(extent))])
    return level


def scatter_about(own_key, shape, scale, bound, pieces=(), kind=jnp.bfloat16):
    entries = scale * jax.random.normal(own_key, shape, jnp.float32)
    if pieces:
        entries = entries * block_levels(own_key, shape, pieces, -0.22, 0.18)
    return jnp.clip(entries, -bound, bound).astype(kind)


def setup_inputs(seed: int = 0) -> dict:
    seeds = jax.random.split(jax.random.key(seed), 12)
    return {
        "feeder_state": scatter_about(seeds[0], (FEEDERS, HOURS, NODES), 1.0, 6.0, ((0, 32),), jnp.float32),
        "feeder_load": scatter_about(seeds[1], (FEEDERS, HOURS, NODES), 1.0, 6.0, ((0, 32),)),
        "feeder_inverse": draw_feeder_inverse(jax.random.fold_in(seeds[11], 71), 0),
        "coupling": scatter_about(seeds[3], (FEEDERS, NODES), NODES ** -0.5, 0.375, ((0, 32),)),
        "feeder_bus": place_ends(jax.random.randint(seeds[4], (FEEDERS,), 0, BUSES), jax.random.fold_in(seeds[4], 1), 0, BUSES - 1).astype(jnp.int32),
        "bus_coupling": scatter_about(seeds[5], (BUSES, BUSES), (BUSES // 4) ** -0.5, 0.1875, ((0, 32),)),
        "bus_diagonal": jnp.clip(1.0 + 2.0 * jax.random.uniform(seeds[6], (BUSES,), jnp.float32) ** block_levels(seeds[6], (BUSES,), ((0, 32),), -0.2, 0.2), 1.0, 3.0),
        "bus_load": scatter_about(seeds[7], (HOURS, BUSES), 1.0, 6.0, ((1, 32),), jnp.float32),
        "bus_state": scatter_about(seeds[8], (HOURS, BUSES), 1.0, 6.0, ((1, 32),), jnp.float32),
        "barrier": jnp.clip(jnp.exp(jax.random.uniform(seeds[9], (ITERS,), jnp.float32, math.log(0.5), math.log(4.0))), 0.5, 4.0),
        "step_length": jnp.clip(jax.random.uniform(seeds[10], (ITERS,), jnp.float32, 0.4, 1.0), 0.4, 1.0),
    }


def feeder_products(blocks, vectors):
    count = vectors.shape[1]
    grouped = blocks.reshape(-1, FEED_DEV, NODES, NODES)
    columns = vectors.reshape(-1, FEED_DEV, count, NODES)

    def one_group(pair_block):
        return jnp.einsum("fij,fhj->fhi", pair_block[0].astype(jnp.float32), pair_block[1].astype(jnp.float32), precision=lax.Precision.HIGHEST)

    solved = lax.map(one_group, (grouped, columns))
    return solved.reshape(-1, count, NODES)


def reference(feeder_state, feeder_load, feeder_inverse, coupling, feeder_bus, bus_coupling, bus_diagonal, bus_load, bus_state, barrier, step_length):
    sensitivity = coupling.astype(jnp.float32)
    response = feeder_products(feeder_inverse, coupling[:, None, :])[:, 0, :]
    schur = jnp.sum(sensitivity * response, axis=-1)
    bus_schur = jax.ops.segment_sum(schur, feeder_bus, BUSES)
    feeder_now = feeder_state
    bus_now = bus_state
    for iteration in range(ITERS):
        weight_mu = barrier[iteration]
        residual = (feeder_load.astype(jnp.float32) + weight_mu * jax.nn.sigmoid(-feeder_now)).astype(jnp.bfloat16)
        solved = feeder_products(feeder_inverse, residual)
        boundary = jnp.sum(solved * sensitivity[:, None, :], axis=-1)
        bus_totals = jax.ops.segment_sum(boundary, feeder_bus, BUSES).T
        bus_right = bus_load + weight_mu * jax.nn.sigmoid(-bus_now) - bus_totals
        pivots = bus_diagonal + weight_mu + bus_schur
        first_sweep = (bus_right / pivots).astype(jnp.bfloat16)
        coupled = jnp.dot(first_sweep, bus_coupling.T, preferred_element_type=jnp.float32)
        second_sweep = (bus_right - coupled) / pivots
        bus_now = bus_now + step_length[iteration] * second_sweep
        at_feeder = second_sweep[:, feeder_bus].T
        feeder_now = feeder_now + step_length[iteration] * (solved - response[:, None, :] * at_feeder[:, :, None])
    return feeder_now, bus_now
```

```python
import functools

import jax
import jax.numpy as jnp
from jax import lax
from jax.experimental import pallas as pl
from jax.experimental.pallas import tpu as pltpu
from jax.sharding import PartitionSpec as P

AXES = ("grp", "dev")
LANES = 128
F32 = jnp.float32
BF16 = jnp.bfloat16


def sigmoid_neg(x):
    return 1.0 / (1.0 + jnp.exp(x))


def split(x):
    high = x.astype(BF16).astype(F32)
    return high, x - high


def lane_iota(rows, lanes=LANES):
    return lax.broadcasted_iota(jnp.int32, (rows, lanes), 1)


def feeder_first(
    block, mu_ref, step_ref, state_ref, load_ref, inverse_ref, coupling_ref, bus_ref,
    diagonal_ref, bus_load_ref, bus_state_ref, partial_ref, response_ref, send_ref, sums_ref, ids_ref,
):
    at = pl.program_id(0)
    hours = state_ref.shape[1]
    mu, step = mu_ref[0], step_ref[0]

    @pl.when(at == 0)
    def _():
        sums_ref[...] = jnp.zeros_like(sums_ref)

    lanes = lane_iota(hours + 8)
    sums = sums_ref[...]
    for k in range(block):
        state = state_ref[k]
        residual = load_ref[k].astype(F32) + mu * sigmoid_neg(state)
        row = jnp.broadcast_to(coupling_ref[pl.ds(k, 1), :].astype(F32), (8, state.shape[1]))
        stacked = jnp.concatenate([residual, row], axis=0).astype(BF16)
        product = jnp.dot(stacked, inverse_ref[k], preferred_element_type=F32)
        response = product[hours : hours + 1]
        partial_ref[k] = state + step * product[:hours]
        response_ref[pl.ds(k, 1), :] = response
        dots = jnp.sum(stacked.astype(F32) * response, axis=1, keepdims=True)
        sums = jnp.where(lanes == at * block + k, dots, sums)
    sums_ref[...] = sums

    @pl.when(at == pl.num_programs(0) - 1)
    def _():
        count = bus_ref.shape[1]
        ids_ref[...] = jnp.full_like(ids_ref, -1)
        ids_ref[0:1, 0:count] = bus_ref[...]
        ids = ids_ref[0:1, :]
        width = 2 * LANES
        schur, schur_low = split(sums_ref[hours : hours + 1, :])
        diag, diag_low = split(diagonal_ref[...])
        rows = lax.broadcasted_iota(jnp.int32, (8, LANES), 0)
        extra = jnp.zeros((8, LANES), F32)
        for at_row, value in enumerate(
            (
                schur,
                schur_low,
                (ids // width).astype(F32),
                (ids % width).astype(F32),
                diag,
                diag_low,
            )
        ):
            extra = jnp.where(rows == at_row, value, extra)
        base = bus_load_ref[...] + mu * sigmoid_neg(bus_state_ref[...])
        message = jnp.concatenate([sums_ref[0:hours, :], extra, base], axis=0).astype(BF16)
        for to in range(send_ref.shape[0]):
            send_ref[to] = message


def digit_columns(ids_ref, first_ref, hours):
    devices = first_ref.shape[0]
    for d in range(devices):
        ids_ref[pl.ds(d, 1), :] = first_ref[d, hours : hours + 8, :].astype(F32)[3:4]
    return ids_ref[...].T


def scatter_buses(totals_ref, ids_ref, first_ref, rows_of, hours):
    digits, height, width = totals_ref.shape
    devices = first_ref.shape[0]
    columns = digit_columns(ids_ref, first_ref, hours)
    low = lax.broadcasted_iota(jnp.int32, (LANES, width), 1).astype(F32)
    for pair in range(devices // 2):
        one_hot, rows, high = [], [], []
        for d in (2 * pair, 2 * pair + 1):
            one_hot.append((columns[:, d : d + 1] == low).astype(F32).astype(BF16))
            rows.append(rows_of(d))
            high.append(first_ref[d, hours : hours + 8, :].astype(F32)[2:3])
        one_hot = jnp.concatenate(one_hot, axis=0)
        rows = jnp.concatenate(rows, axis=1)
        high = jnp.concatenate(high, axis=1)
        picked = jnp.concatenate(
            [jnp.where(high == float(h), rows, 0.0) for h in range(digits)], axis=0
        ).astype(BF16)
        part = jnp.dot(picked, one_hot, preferred_element_type=F32).reshape(digits, height, width)
        if pair == 0:
            totals_ref[...] = part
        else:
            totals_ref[...] += part


def bus_kernel(
    iteration, last, hours, me_ref, mu_ref, step_ref, first_ref, rows_ref, base_ref, bus_coupling_ref,
    diagonal_ref, bus_load_ref, bus_state_ref, schur_in_ref, send_ref, state_out_ref, schur_out_ref,
    totals_ref, ids_ref,
):
    me = me_ref[0]
    mu, step = mu_ref[iteration], step_ref[iteration]
    digits, height, width = totals_ref.shape
    rows_of = lambda d: rows_ref[d, 0:height, :].astype(F32)
    scatter_buses(totals_ref, ids_ref, first_ref, rows_of, hours)
    base_at = base_ref.shape[1] - hours
    coupled = jnp.zeros((hours, bus_coupling_ref.shape[0]), F32)
    for h in range(digits):
        totals = totals_ref[h]
        pair = (2 * h, 2 * h + 1)
        base = jnp.concatenate([base_ref[d, base_at:, :].astype(F32) for d in pair], axis=1)
        extra = jnp.concatenate([first_ref[d, hours : hours + 8, :].astype(F32) for d in pair], axis=1)
        if iteration == 0:
            schur = totals[hours : hours + 1] + totals[hours + 1 : hours + 2]
            schur_out_ref[pl.ds(h, 1), :] = schur
        else:
            schur = schur_in_ref[pl.ds(h, 1), :]
        pivots = extra[4:5] + extra[5:6] + (mu + schur)
        sweep = ((base - totals[:hours]) / pivots).astype(BF16)
        coupled += lax.dot_general(
            sweep,
            bus_coupling_ref[:, h * width : (h + 1) * width],
            (((1,), (1,)), ((), ())),
            preferred_element_type=F32,
        )
    mine = totals_ref[me // 2]
    if iteration == 0:
        schur = mine[hours : hours + 1] + mine[hours + 1 : hours + 2]
    else:
        schur = schur_in_ref[pl.ds(me // 2, 1), :]
    odd = lax.rem(me, 2) == 1
    half = lambda x: jnp.where(odd, x[:, LANES:], x[:, :LANES])
    state = bus_state_ref[...]
    right = bus_load_ref[...] + mu * sigmoid_neg(state) - half(mine)[:hours]
    second = (right - coupled) / (diagonal_ref[...] + mu + half(schur))
    state = state + step * second
    state_out_ref[...] = state
    parts = [second]
    if not last:
        parts.append(bus_load_ref[...] + mu_ref[iteration + 1] * sigmoid_neg(state))
    message = jnp.concatenate(parts, axis=0).astype(BF16)
    for to in range(send_ref.shape[0]):
        send_ref[to] = message


def feeder_middle(
    block, iteration, mu_ref, step_ref, bus_ref, sweep_ref, partial_ref, load_ref, response_ref,
    residual_ref, send_ref, sums_ref,
):
    at = pl.program_id(0)
    hours = load_ref.shape[1]
    mu, step = mu_ref[iteration + 1], step_ref[iteration]

    @pl.when(at == 0)
    def _():
        sums_ref[...] = jnp.zeros_like(sums_ref)

    lanes = lane_iota(hours)
    sums = sums_ref[...]
    for k in range(block):
        bus = bus_ref[at * block + k]
        tile = sweep_ref[bus // LANES, 0:hours, :].astype(F32)
        column = jnp.sum(jnp.where(lanes == bus % LANES, tile, 0.0), axis=1, keepdims=True)
        response = response_ref[pl.ds(k, 1), :]
        state = partial_ref[k] - response * (step * column)
        residual = (load_ref[k].astype(F32) + mu * sigmoid_neg(state)).astype(BF16)
        residual_ref[k] = residual
        dots = jnp.sum(residual.astype(F32) * response, axis=1, keepdims=True)
        sums = jnp.where(lanes == at * block + k, dots, sums)
    sums_ref[...] = sums

    @pl.when(at == pl.num_programs(0) - 1)
    def _():
        message = sums_ref[...].astype(BF16)
        for to in range(send_ref.shape[0]):
            send_ref[to] = message


def feeder_last(
    block, step_ref, bus_ref, first_sweep_ref, second_sweep_ref, partial_ref, residual_ref, inverse_ref,
    response_ref, out_ref,
):
    at = pl.program_id(0)
    hours = partial_ref.shape[1]
    lanes = lane_iota(hours)
    for k in range(block):
        bus = bus_ref[at * block + k]
        tile = step_ref[0] * first_sweep_ref[bus // LANES, 0:hours, :].astype(F32)
        tile += step_ref[1] * second_sweep_ref[bus // LANES, 0:hours, :].astype(F32)
        column = jnp.sum(jnp.where(lanes == bus % LANES, tile, 0.0), axis=1, keepdims=True)
        solved = jnp.dot(residual_ref[k], inverse_ref[k], preferred_element_type=F32)
        out_ref[k] = partial_ref[k] + step_ref[1] * solved - response_ref[pl.ds(k, 1), :] * column


def spread(message):
    return lax.all_to_all(message, AXES, 0, 0, tiled=True)


SMEM = pl.BlockSpec(memory_space=pltpu.SMEM)
VMEM = pl.BlockSpec(memory_space=pltpu.VMEM)
LIMIT = 32 * 1024 * 1024


def on_device(
    devices, feeder_state, feeder_load, feeder_inverse, coupling, feeder_bus, bus_coupling, bus_diagonal,
    bus_load, bus_state, barrier, step_length,
):
    feeders, hours, nodes = feeder_state.shape
    own, buses = bus_coupling.shape
    width = 2 * LANES
    digits = buses // width
    block = 8
    steps = feeders // block
    me = lax.axis_index(AXES).astype(jnp.int32)[None]
    diagonal = bus_diagonal[None, :]
    whole = lambda *shape: pl.BlockSpec(shape, lambda i: (0,) * len(shape))
    cube = pl.BlockSpec((block, hours, nodes), lambda i: (i, 0, 0))
    square = pl.BlockSpec((block, nodes, nodes), lambda i: (i, 0, 0))
    flat = pl.BlockSpec((block, nodes), lambda i: (i, 0))
    params = pltpu.CompilerParams(dimension_semantics=("arbitrary",), vmem_limit_bytes=LIMIT)
    shape = jax.ShapeDtypeStruct

    partial, response, message = pl.pallas_call(
        functools.partial(feeder_first, block),
        grid=(steps,),
        in_specs=[
            SMEM, SMEM, cube, cube, square, flat, whole(1, feeders), whole(1, own), whole(hours, own),
            whole(hours, own),
        ],
        out_specs=[cube, flat, whole(devices, 2 * hours + 8, LANES)],
        out_shape=[
            shape((feeders, hours, nodes), F32),
            shape((feeders, nodes), F32),
            shape((devices, 2 * hours + 8, LANES), BF16),
        ],
        scratch_shapes=[pltpu.VMEM((hours + 8, LANES), F32), pltpu.VMEM((8, LANES), jnp.int32)],
        compiler_params=params,
        name="feeder_first",
    )(
        barrier, step_length, feeder_state, feeder_load, feeder_inverse, coupling, feeder_bus[None, :],
        diagonal, bus_load, bus_state,
    )
    first = spread(message)

    def bus_call(iteration, rows, base, height, state, schur):
        last = iteration == barrier.shape[0] - 1
        out_rows = hours if last else 2 * hours
        return pl.pallas_call(
            functools.partial(bus_kernel, iteration, last, hours),
            in_specs=[SMEM] * 3 + [VMEM] * 8,
            out_specs=[VMEM] * 3,
            out_shape=[
                shape((devices, out_rows, LANES), BF16),
                shape((hours, own), F32),
                shape((digits, width), F32),
            ],
            scratch_shapes=[
                pltpu.VMEM((digits, height, width), F32),
                pltpu.VMEM((devices, LANES), F32),
            ],
            compiler_params=pltpu.CompilerParams(vmem_limit_bytes=(12 + 3 * devices // 10) << 20),
            name=f"bus_sweeps_{iteration}",
        )(me, barrier, step_length, first, rows, base, bus_coupling, diagonal, bus_load, state, schur)

    message, bus_now, schur = bus_call(
        0, first, first, hours + 8, bus_state, jnp.zeros((digits, width), F32)
    )
    sweep_first = spread(message)

    residual, message = pl.pallas_call(
        functools.partial(feeder_middle, block, 0),
        grid=(steps,),
        in_specs=[SMEM, SMEM, SMEM, whole(devices, 2 * hours, LANES), cube, cube, flat],
        out_specs=[cube, whole(devices, hours, LANES)],
        out_shape=[shape((feeders, hours, nodes), BF16), shape((devices, hours, LANES), BF16)],
        scratch_shapes=[pltpu.VMEM((hours, LANES), F32)],
        compiler_params=params,
        name="feeder_middle",
    )(barrier, step_length, feeder_bus, sweep_first, partial, feeder_load, response)
    rows = spread(message)

    message, bus_now, _ = bus_call(1, rows, sweep_first, hours, bus_now, schur)
    sweep_second = spread(message)

    feeder_now = pl.pallas_call(
        functools.partial(feeder_last, block),
        grid=(steps,),
        in_specs=[
            SMEM, SMEM, whole(devices, 2 * hours, LANES), whole(devices, hours, LANES), cube, cube, square,
            flat,
        ],
        out_specs=cube,
        out_shape=shape((feeders, hours, nodes), F32),
        compiler_params=params,
        name="feeder_last",
    )(step_length, feeder_bus, sweep_first, sweep_second, partial, residual, feeder_inverse, response)
    return feeder_now, bus_now


def solution(mesh):
    devices = mesh.shape["grp"] * mesh.shape["dev"]
    in_specs = (
        P(AXES, None, None),
        P(AXES, None, None),
        P(AXES, None, None),
        P(AXES, None),
        P(AXES),
        P(AXES, None),
        P(AXES),
        P(None, AXES),
        P(None, AXES),
        P(),
        P(),
    )
    out_specs = (P(AXES, None, None), P(None, AXES))
    return jax.shard_map(
        functools.partial(on_device, devices), mesh=mesh, in_specs=in_specs, out_specs=out_specs,
        check_vma=False,
    )
```
